32 devices in a mesh: row: 4 (over y, x), col: 8 (over z, core).
Axes of the slice: x: 2, y: 2, z: 4, core: 2. Of those that a mesh axis runs over, the one named last changes fastest.
Arguments:
- basis: bfloat16 [40, 131072], P(None, ('row', 'col'))
- expand: float32 [3, 8, 40], replicated, may hold values from -1 to 1
- tiles: bfloat16 [3, 3072, 128, 128], P(None, ('row', 'col')), may hold values from -0.3125 to 0.3125
- tile_rows: int32 [3072], P(('row', 'col')), may hold values from 0 to 255, as said below
- tile_cols: int32 [3072], P(('row', 'col')), may hold values from 0 to 127
Outputs:
- new_block: float32 [8, 131072], P(None, ('row', 'col'))
- coefficients: float32 [8, 40], replicated
- factor: float32 [8, 8], replicated
The draws below stay inside these ranges and needn't reach their ends.
Inputs may be any that keep to these rules, and one draw needn't show every extreme that they name: `tile_rows`: each device's 96 tiles come in 8 runs of 12; the row tiles of run k are 12 distinct values from k * 32 to (k + 1) * 32 - 1.
All inputs are finite; a program needn't handle non-finite values.
Results may differ from the reference program's by a relative error of at most 0.0054.
Values may be sent and summed in bfloat16 or wider, within the bound.
A program may use at most 64 MiB of HBM per device.

```python
import math
import jax
import jax.numpy as jnp
from jax import lax

LOC = 4096
CAP = 12
TILE = 128
KD = 40
BS = 8
TPD = 96
NTOT = 131072
N_ROW = 4
N_COL = 8


def draw_basis(key, part):
    key_noise, key_common, key_lean = jax.random.split(key, 3)
    random_part = jax.random.normal(key_noise, (KD, NTOT), jnp.float32)
    common = jax.random.normal(key_common, (NTOT,), jnp.float32)
    leaning = jax.random.uniform(key_lean, (KD,), jnp.float32, -0.7, 0.7)
    return (random_part + leaning[:, None] * common[None, :]).astype(jnp.bfloat16)


def draw_tile_rows(key, part):
    region = LOC // TILE
    runs = N_ROW * N_COL * N_COL
    subkeys = jax.random.split(jax.random.fold_in(key, 7), runs)
    chosen = jax.vmap(lambda subkey: jax.random.permutation(subkey, region))(subkeys)[:, :CAP]
    offsets = jnp.arange(runs, dtype=jnp.int32) % N_COL * region
    return (chosen.astype(jnp.int32) + offsets[:, None]).reshape(runs * CAP).astype(jnp.int32)


def with_ends(array, stream_key, smallest, high):
    extent = array.shape
    place = [jax.random.randint(jax.random.fold_in(stream_key, axis), (), 0, extent[axis]) for axis in range(len(extent))]
    array = array.at[tuple(place)].set(smallest)
    longest = extent.index(max(extent))
    place[longest] = (place[longest] + 1) % extent[longest]
    return array.at[tuple(place)].set(high)


def block_scale(key, extent, shards, least, high):
    def one(dim, blocks):
        heights = jax.random.uniform(jax.random.fold_in(jax.random.fold_in(key, 6), dim), (blocks,), jnp.float32, least / len(shards), high / len(shards))
        return jnp.repeat(jnp.exp(heights), extent[dim] // blocks).reshape((-1,) + (1,) * (len(extent) - dim - 1))

    factor_of = one(*shards[0])
    for cut in shards[1:]:
        factor_of = factor_of * one(*cut)
    return factor_of


def noise(key, shape, scale, reach, pieces=(), kind=jnp.bfloat16):
    values = jax.random.normal(key, shape, jnp.float32) * scale
    if len(pieces) > 0:
        values = block_scale(key, shape, pieces, -0.22, 0.18) * values
    return jnp.clip(values, min=-reach, max=reach).astype(kind)


def setup_inputs(seed: int = 0) -> dict:
    key_of = jax.random.split(jax.random.key(seed), 6)
    return {
        "basis": draw_basis(jax.random.fold_in(key_of[5], 71), 0),
        "expand": noise(key_of[1], (3, BS, KD), KD ** -0.5, 1.0, (), jnp.float32),
        "tiles": noise(key_of[2], (3, TPD * N_ROW * N_COL, TILE, TILE), (TPD * TILE * TILE // LOC) ** -0.5, 0.3125, ((1, 32),)),
        "tile_rows": draw_tile_rows(jax.random.fold_in(key_of[5], 71), 0),
        "tile_cols": with_ends(jax.random.randint(key_of[4], (TPD * N_ROW * N_COL,), 0, N_ROW * LOC // TILE), jax.random.fold_in(key_of[4], 1), 0, (N_ROW * LOC // TILE) - 1).astype(jnp.int32),
    }


def reference(basis, expand, tiles, tile_rows, tile_cols):
    entries = LOC * N_ROW * N_COL
    inverse_root = 1.0 / math.sqrt(entries)
    highest = lax.Precision.HIGHEST
    basis_full = basis.astype(jnp.float32)
    series = jnp.einsum('mbk,kn->mbn', expand.astype(jnp.float32), basis_full, precision=highest).astype(jnp.bfloat16)
    layout = series.reshape(3, BS, N_ROW, N_COL, LOC)
    region = LOC // TILE
    slot_count = N_COL * region

    def device(index_dev, sums_row):
        index_dev = index_dev.astype(jnp.int32)
        row_index = index_dev // N_COL
        col_index = index_dev % N_COL
        columns = lax.dynamic_index_in_dim(layout, col_index, 3, keepdims=False)
        columns = columns.reshape(3, BS, N_ROW * LOC // TILE, TILE)
        start = (index_dev * TPD).astype(jnp.int32)
        matrices = lax.dynamic_slice_in_dim(tiles, start, TPD, 1).astype(jnp.float32)
        rows_here = lax.dynamic_slice_in_dim(tile_rows, start, TPD, 0)
        cols_here = lax.dynamic_slice_in_dim(tile_cols, start, TPD, 0)
        picked = jnp.take(columns, cols_here, axis=2).astype(jnp.float32)
        products = jnp.einsum('mtij,mbtj->bti', matrices, picked, precision=highest)
        onehot = (rows_here[:, None] == jnp.arange(slot_count, dtype=jnp.int32)[None, :]).astype(jnp.float32)
        partial_value = jnp.einsum('ts,bti->bsi', onehot, products, precision=highest).reshape(BS, slot_count * TILE)
        return sums_row.at[:, row_index].add(partial_value)
    sums_row = lax.fori_loop(0, N_ROW * N_COL, device, jnp.zeros((BS, N_ROW, slot_count * TILE), jnp.float32))
    applied = sums_row.reshape(BS, entries)
    first_pass = jnp.dot(applied, basis_full.T, precision=highest) * inverse_root
    projected = applied - jnp.dot(first_pass, basis_full, precision=highest) * inverse_root
    second_pass = jnp.dot(projected, basis_full.T, precision=highest) * inverse_root
    cleaned = projected - jnp.dot(second_pass, basis_full, precision=highest) * inverse_root
    coefficients = first_pass + second_pass
    gram_block = jnp.dot(cleaned, cleaned.T, precision=highest) / entries
    factor = jnp.linalg.cholesky(gram_block)
    new_block = lax.linalg.triangular_solve(factor, cleaned, left_side=True, lower=True)
    return (new_block, coefficients, factor)
```

```python
import functools
import math

import jax
import jax.numpy as jnp
from jax import lax
from jax.experimental import pallas as pl
from jax.experimental.pallas import tpu as pltpu
from jax.sharding import PartitionSpec as P

F32 = jnp.float32
BF16 = jnp.bfloat16
NT = (((1,), (1,)), ((), ()))


def exact(a, b, dims=(((1,), (0,)), ((), ()))):
    return lax.dot_general(a, b, dims, precision=lax.Precision.HIGHEST, preferred_element_type=F32)


def pieces(x):
    one = x.astype(BF16).astype(F32)
    rest = x - one
    two = rest.astype(BF16).astype(F32)
    three = rest - two
    return jnp.concatenate([one, two, three], axis=0).astype(BF16)


def fold(x, rows):
    return x[:rows] + x[rows : 2 * rows] + x[2 * rows :]


def kernel(
    nrow,
    ncol,
    expand_ref,
    rows_ref,
    picks_ref,
    basis_hbm,
    tiles_hbm,
    new_ref,
    coef_ref,
    factor_ref,
    basis,
    tiles,
    cols,
    outbox,
    inbox,
    seg_out,
    seg_in,
    corr_col,
    corr_row,
    tail_col,
    tail_row,
    spread,
    app,
    basis_sem,
    tile_sem,
    ser_send,
    ser_recv,
    seg_send,
    seg_recv,
    box_send,
    box_recv,
    cc_send,
    cc_recv,
    cr_send,
    cr_recv,
    tc_send,
    tc_recv,
    tr_send,
    tr_recv,
):
    r = lax.axis_index("row")
    c = lax.axis_index("col")
    krylov, length = basis.shape
    kinds, tpd, tile, _ = tiles.shape
    cap = tpd // ncol
    region = length // tile
    bs = expand_ref.shape[1]
    entries = length * nrow * ncol
    inverse_root = 1.0 / math.sqrt(entries)
    width = seg_in.shape[2]

    load_basis = pltpu.make_async_copy(basis_hbm, basis, basis_sem)
    load_basis.start()

    def chunk_copy(m, k):
        part = pl.ds(k * cap, cap)
        return pltpu.make_async_copy(tiles_hbm.at[m, part], tiles.at[m, part], tile_sem.at[m, k])

    for j in range(1, ncol + 1):
        k = lax.rem(c + j, ncol)
        for m in range(kinds):
            chunk_copy(m, k).start()

    barrier = pltpu.get_barrier_semaphore()
    for j in range(1, nrow):
        pl.semaphore_signal(barrier, inc=1, device_id={"row": lax.rem(r + j, nrow)}, device_id_type=pl.DeviceIdType.MESH)
    for j in range(1, ncol):
        pl.semaphore_signal(barrier, inc=1, device_id={"col": lax.rem(c + j, ncol)}, device_id_type=pl.DeviceIdType.MESH)

    def remote(src, dst, send_sem, recv_sem, where):
        return pltpu.make_async_remote_copy(
            src_ref=src, dst_ref=dst, send_sem=send_sem, recv_sem=recv_sem,
            device_id=where, device_id_type=pl.DeviceIdType.MESH,
        )

    def row_at(j):
        peer = lax.rem(r + j, nrow)
        return peer, {"row": peer}

    def col_at(j):
        peer = lax.rem(c + j, ncol)
        return peer, {"col": peer}

    load_basis.wait()
    expand = pieces(expand_ref[...].reshape(kinds * bs, krylov))
    for l in range(region):
        part = fold(jnp.dot(expand, basis[:, l * tile : (l + 1) * tile], preferred_element_type=F32), kinds * bs)
        for m in range(kinds):
            cols[m, r * region + l] = part[m * bs : (m + 1) * bs].astype(BF16)

    pl.semaphore_wait(barrier, nrow + ncol - 2)

    def series_copy(m, owner, peer, where):
        block = cols.at[m, pl.ds(owner * region, region)]
        return remote(block, block, ser_send.at[m, peer], ser_recv.at[m, owner], where)

    for m in range(kinds):
        for j in range(1, nrow):
            peer, where = row_at(j)
            series_copy(m, r, peer, where).start()

    slot = lax.broadcasted_iota(jnp.int32, (1, width), 1)
    for k in range(ncol):
        line = jnp.zeros((1, width), jnp.int32)
        for t in range(cap):
            line = jnp.where(lax.rem(slot, cap) == t, rows_ref[k * cap + t], line)
        seg_out[k] = line
    for j in range(1, ncol):
        peer, where = col_at(j)
        remote(seg_out.at[peer], seg_in.at[c], seg_send.at[peer], seg_recv.at[c], where).start()
    seg_in[c] = seg_out[c]

    corr_col[c] = jnp.pad(
        lax.dot_general(basis[...], basis[...], NT, preferred_element_type=F32), ((0, 0), (0, 128 - krylov))
    )
    for j in range(1, ncol):
        peer, where = col_at(j)
        remote(corr_col.at[c], corr_col.at[c], cc_send.at[peer], cc_recv.at[c], where).start()

    for m in range(kinds):
        for j in range(1, nrow):
            peer, where = row_at(j)
            series_copy(m, peer, peer, where).wait_recv()

    def products(k, dst):
        for m in range(kinds):
            chunk_copy(m, k).wait()
        for t in range(cap):
            g = k * cap + t
            at = picks_ref[g]
            x = jnp.concatenate([cols[m, at] for m in range(kinds)], axis=1)
            w = jnp.concatenate([tiles[m, g] for m in range(kinds)], axis=1)
            dst[k, t] = lax.dot_general(x, w, NT, preferred_element_type=F32).astype(BF16)

    def box_copy(k, where):
        return remote(outbox.at[k], inbox.at[c], box_send.at[k], box_recv.at[c], where)

    def chunk(j, carry):
        k, where = col_at(j)
        products(k, outbox)
        box_copy(k, where).start()
        return carry

    lax.fori_loop(1, ncol, chunk, 0)
    products(c, inbox)

    for j in range(1, ncol):
        peer, where = col_at(j)
        remote(corr_col.at[c], corr_col.at[peer], cc_send.at[peer], cc_recv.at[peer], where).wait_recv()
    corr_row[r] = jnp.sum(corr_col[...], axis=0)
    for j in range(1, nrow):
        peer, where = row_at(j)
        remote(corr_row.at[r], corr_row.at[r], cr_send.at[peer], cr_recv.at[r], where).start()

    for j in range(1, ncol):
        peer, where = col_at(j)
        remote(seg_out.at[peer], seg_in.at[peer], seg_send.at[peer], seg_recv.at[peer], where).wait_recv()
    line = seg_in[0]
    for k in range(1, ncol):
        line = jnp.where(lax.div(slot, cap) == k, seg_in[k], line)
    here = lax.broadcasted_iota(jnp.int32, (region, tpd), 0) + c * region
    onehot = (line[:, :tpd] == here).astype(F32).astype(BF16)

    for j in range(1, nrow):
        peer, where = row_at(j)
        remote(corr_row.at[r], corr_row.at[peer], cr_send.at[peer], cr_recv.at[peer], where).wait_recv()
    corr = jnp.sum(corr_row[...], axis=0)[:, :krylov] / entries
    eye = (
        lax.broadcasted_iota(jnp.int32, (krylov, krylov), 0) == lax.broadcasted_iota(jnp.int32, (krylov, krylov), 1)
    ).astype(F32)
    once = eye - corr
    both = eye + once
    kern = exact(both, eye + exact(once, once))

    for j in range(1, ncol):
        peer, where = col_at(j)
        remote(outbox.at[peer], inbox.at[peer], box_send.at[peer], box_recv.at[peer], where).wait_recv()
    spread[...] = inbox[...].astype(F32).reshape(tpd, bs, tile)
    for b in range(bs):
        app[:, b, :] = jnp.dot(onehot, spread[:, b, :].astype(BF16), preferred_element_type=F32)
    applied = jnp.concatenate([app[s] for s in range(region)], axis=1)

    split = pieces(applied)
    raw = fold(lax.dot_general(split, basis[...], NT, preferred_element_type=F32), bs)
    energy = fold(lax.dot_general(split, split, NT, preferred_element_type=F32), bs)
    energy = energy[:, :bs] + energy[:, bs : 2 * bs] + energy[:, 2 * bs :]
    tail_col[c] = jnp.concatenate([raw, energy, jnp.zeros((bs, 128 - krylov - bs), F32)], axis=1)
    for j in range(1, ncol):
        peer, where = col_at(j)
        remote(tail_col.at[c], tail_col.at[c], tc_send.at[peer], tc_recv.at[c], where).start()
    for j in range(1, ncol):
        peer, where = col_at(j)
        remote(tail_col.at[c], tail_col.at[peer], tc_send.at[peer], tc_recv.at[peer], where).wait_recv()
    tail_row[r] = jnp.sum(tail_col[...], axis=0)
    for j in range(1, nrow):
        peer, where = row_at(j)
        remote(tail_row.at[r], tail_row.at[r], tr_send.at[peer], tr_recv.at[r], where).start()
    for j in range(1, nrow):
        peer, where = row_at(j)
        remote(tail_row.at[r], tail_row.at[peer], tr_send.at[peer], tr_recv.at[peer], where).wait_recv()
    total = jnp.sum(tail_row[...], axis=0)

    first = total[:, :krylov] * inverse_root
    coefficients = exact(first, both)
    gram = (total[:, krylov : krylov + bs] - exact(exact(first, kern), first, NT)) / entries
    coef_ref[...] = coefficients

    sub = lax.broadcasted_iota(jnp.int32, (bs, bs), 0)
    lane = lax.broadcasted_iota(jnp.int32, (bs, bs), 1)
    up = lax.broadcasted_iota(jnp.int32, (bs, 1), 0)
    factor = jnp.zeros((bs, bs), F32)
    inverse = jnp.zeros((bs, 1), F32)
    steps = []
    for j in range(bs):
        column, line = gram[:, j : j + 1], gram[j : j + 1, :]
        pivot = jnp.sqrt(gram[j : j + 1, j : j + 1])
        column = jnp.where(up >= j, column / pivot, 0.0)
        factor = jnp.where(lane == j, column, factor)
        inverse = jnp.where(up == j, 1.0 / pivot, inverse)
        steps.append(jnp.where(up > j, column, 0.0))
        gram = gram - column * (line / pivot)
    factor_ref[...] = factor

    cleaned = applied - fold(
        jnp.dot(pieces(coefficients * inverse_root), basis[...], preferred_element_type=F32), bs
    )
    solved = cleaned * inverse
    for j in range(bs - 1):
        solved = solved - (steps[j] * inverse) * solved[j : j + 1, :]
    new_ref[...] = solved

    for m in range(kinds):
        for j in range(1, nrow):
            peer, where = row_at(j)
            series_copy(m, r, peer, where).wait_send()
    for j in range(1, ncol):
        peer, where = col_at(j)
        remote(seg_out.at[peer], seg_in.at[c], seg_send.at[peer], seg_recv.at[c], where).wait_send()
        remote(corr_col.at[c], corr_col.at[c], cc_send.at[peer], cc_recv.at[c], where).wait_send()
        box_copy(peer, where).wait_send()
        remote(tail_col.at[c], tail_col.at[c], tc_send.at[peer], tc_recv.at[c], where).wait_send()
    for j in range(1, nrow):
        peer, where = row_at(j)
        remote(corr_row.at[r], corr_row.at[r], cr_send.at[peer], cr_recv.at[r], where).wait_send()
        remote(tail_row.at[r], tail_row.at[r], tr_send.at[peer], tr_recv.at[r], where).wait_send()


def shards(basis, expand, tiles, tile_rows, tile_cols):
    nrow = lax.axis_size("row")
    ncol = lax.axis_size("col")
    krylov, length = basis.shape
    kinds, tpd, tile, _ = tiles.shape
    bs = expand.shape[1]
    region = length // tile
    cap = tpd // ncol
    width = -(-tpd // 128) * 128
    dma = pltpu.SemaphoreType.DMA
    vmem, smem = pl.BlockSpec(memory_space=pltpu.VMEM), pl.BlockSpec(memory_space=pltpu.SMEM)
    hbm = pl.BlockSpec(memory_space=pl.ANY)
    return pl.pallas_call(
        functools.partial(kernel, nrow, ncol),
        out_shape=(
            jax.ShapeDtypeStruct((bs, length), F32),
            jax.ShapeDtypeStruct((bs, krylov), F32),
            jax.ShapeDtypeStruct((bs, bs), F32),
        ),
        in_specs=[vmem, smem, smem, hbm, hbm],
        out_specs=(vmem, vmem, vmem),
        scratch_shapes=[
            pltpu.VMEM((krylov, length), BF16),
            pltpu.VMEM((kinds, tpd, tile, tile), BF16),
            pltpu.VMEM((kinds, nrow * region, bs, tile), BF16),
            pltpu.VMEM((ncol, cap, bs, tile), BF16),
            pltpu.VMEM((ncol, cap, bs, tile), BF16),
            pltpu.VMEM((ncol, 1, width), jnp.int32),
            pltpu.VMEM((ncol, 1, width), jnp.int32),
            pltpu.VMEM((ncol, krylov, 128), F32),
            pltpu.VMEM((nrow, krylov, 128), F32),
            pltpu.VMEM((ncol, bs, 128), F32),
            pltpu.VMEM((nrow, bs, 128), F32),
            pltpu.VMEM((tpd, bs, tile), F32),
            pltpu.VMEM((region, bs, tile), F32),
            dma,
            dma((kinds, ncol)),
            dma((kinds, nrow)),
            dma((kinds, nrow)),
            dma((ncol,)),
            dma((ncol,)),
            dma((ncol,)),
            dma((ncol,)),
            dma((ncol,)),
            dma((ncol,)),
            dma((nrow,)),
            dma((nrow,)),
            dma((ncol,)),
            dma((ncol,)),
            dma((nrow,)),
            dma((nrow,)),
        ],
        compiler_params=pltpu.CompilerParams(
            collective_id=0, has_side_effects=True, vmem_limit_bytes=48 * 1024 * 1024
        ),
    )(expand, tile_rows, tile_cols, basis, tiles)


def solution(mesh):
    return jax.shard_map(
        shards,
        mesh=mesh,
        in_specs=(
            P(None, ("row", "col")),
            P(),
            P(None, ("row", "col"), None, None),
            P(("row", "col")),
            P(("row", "col")),
        ),
        out_specs=(P(None, ("row", "col")), P(), P()),
        check_vma=False,
    )
```

```python
import functools
import math

import jax
import jax.numpy as jnp
from jax import lax
from jax.experimental import pallas as pl
from jax.experimental.pallas import tpu as pltpu
from jax.sharding import PartitionSpec as P

F32 = jnp.float32
BF16 = jnp.bfloat16
NT = (((1,), (1,)), ((), ()))


def exact(a, b, dims=(((1,), (0,)), ((), ()))):
    return lax.dot_general(a, b, dims, precision=lax.Precision.HIGHEST, preferred_element_type=F32)


def pieces(x):
    one = x.astype(BF16).astype(F32)
    rest = x - one
    two = rest.astype(BF16).astype(F32)
    three = rest - two
    return jnp.concatenate([one, two, three], axis=0).astype(BF16)


def fold(x, rows):
    return x[:rows] + x[rows : 2 * rows] + x[2 * rows :]


def kernel(
    nrow,
    ncol,
    expand_hbm,
    rows_hbm,
    picks_hbm,
    basis_hbm,
    tiles_hbm,
    new_ref,
    coef_ref,
    factor_ref,
    expand_ref,
    rows_ref,
    picks_ref,
    basis,
    tiles,
    cols,
    outbox,
    inbox,
    seg_out,
    seg_in,
    corr_col,
    corr_row,
    tail_col,
    tail_row,
    spread,
    app,
    small_sem,
    basis_sem,
    tile_sem,
    ser_send,
    ser_recv,
    fwd_send,
    fwd_recv,
    seg_send,
    seg_recv,
    box_send,
    box_recv,
    cc_send,
    cc_recv,
    cr_send,
    cr_recv,
    tc_send,
    tc_recv,
    tr_send,
    tr_recv,
):
    r = lax.axis_index("row")
    c = lax.axis_index("col")
    krylov, length = basis.shape
    kinds, tpd, tile, _ = tiles.shape
    cap = tpd // ncol
    region = length // tile
    bs = expand_ref.shape[1]
    entries = length * nrow * ncol
    inverse_root = 1.0 / math.sqrt(entries)
    width = seg_in.shape[2]

    load_basis = pltpu.make_async_copy(basis_hbm, basis, basis_sem)
    load_basis.start()
    small = [
        pltpu.make_async_copy(src, dst, small_sem.at[i])
        for i, (src, dst) in enumerate(((expand_hbm, expand_ref), (rows_hbm, rows_ref), (picks_hbm, picks_ref)))
    ]
    for copy in small:
        copy.start()

    def chunk_copy(m, k):
        part = pl.ds(k * cap, cap)
        return pltpu.make_async_copy(tiles_hbm.at[m, part], tiles.at[m, part], tile_sem.at[m, k])

    for j in range(1, ncol + 1):
        k = lax.rem(c + j, ncol)
        for m in range(kinds):
            chunk_copy(m, k).start()

    barrier = pltpu.get_barrier_semaphore()
    for j in range(1, nrow):
        pl.semaphore_signal(barrier, inc=1, device_id={"row": lax.rem(r + j, nrow)}, device_id_type=pl.DeviceIdType.MESH)
    for j in range(1, ncol):
        pl.semaphore_signal(barrier, inc=1, device_id={"col": lax.rem(c + j, ncol)}, device_id_type=pl.DeviceIdType.MESH)

    def remote(src, dst, send_sem, recv_sem, where):
        return pltpu.make_async_remote_copy(
            src_ref=src, dst_ref=dst, send_sem=send_sem, recv_sem=recv_sem,
            device_id=where, device_id_type=pl.DeviceIdType.MESH,
        )

    def row_at(j):
        peer = lax.rem(r + j, nrow)
        return peer, {"row": peer}

    def col_at(j):
        peer = lax.rem(c + j, ncol)
        return peer, {"col": peer}

    for copy in small:
        copy.wait()
    load_basis.wait()
    expand = pieces(expand_ref[...].reshape(kinds * bs, krylov))
    for l in range(region):
        part = fold(jnp.dot(expand, basis[:, l * tile : (l + 1) * tile], preferred_element_type=F32), kinds * bs)
        for m in range(kinds):
            cols[m, r * region + l] = part[m * bs : (m + 1) * bs].astype(BF16)

    pl.semaphore_wait(barrier, nrow + ncol - 2)

    outer = nrow // 2
    side, pair = lax.rem(r, 2), lax.div(r, 2)
    mate = r + 1 - 2 * side
    others = [2 * lax.rem(pair + j, outer) + side for j in range(1, outer)]
    half = region // 2

    def series_copy(m, owner, peer):
        block = cols.at[m, pl.ds(owner * region, region)]
        return remote(block, block, ser_send.at[m, peer], ser_recv.at[m, owner], {"row": peer})

    def pass_on(m, owner, h, peer, slot):
        block = cols.at[m, pl.ds(owner * region + h * half, half)]
        return remote(block, block, fwd_send.at[m, slot, h], fwd_recv.at[m, owner, h], {"row": peer})

    direct = [mate] + others
    for m in range(kinds):
        for peer in direct:
            series_copy(m, r, peer).start()

    slot = lax.broadcasted_iota(jnp.int32, (1, width), 1)
    for k in range(ncol):
        line = jnp.zeros((1, width), jnp.int32)
        for t in range(cap):
            line = jnp.where(lax.rem(slot, cap) == t, rows_ref[k * cap + t], line)
        seg_out[k] = line
    for j in range(1, ncol):
        peer, where = col_at(j)
        remote(seg_out.at[peer], seg_in.at[c], seg_send.at[peer], seg_recv.at[c], where).start()
    seg_in[c] = seg_out[c]

    corr = lax.dot_general(basis[...], basis[...], NT, preferred_element_type=F32)
    band = corr_col.shape[1]
    lanes = corr_col.shape[2]
    folds = -(-krylov // band)
    corr = jnp.pad(corr, ((0, folds * band - krylov), (0, 0)))
    corr_col[c] = jnp.concatenate(
        [corr[i * band : (i + 1) * band] for i in range(folds)] + [jnp.zeros((band, lanes - folds * krylov), F32)], axis=1
    )
    for j in range(1, ncol):
        peer, where = col_at(j)
        remote(corr_col.at[c], corr_col.at[c], cc_send.at[peer], cc_recv.at[c], where).start()

    def relay(m):
        series_copy(m, mate, mate).wait_recv()
        for other in others:
            pass_on(m, mate, 1, other, other).start()
        for other in others:
            series_copy(m, other, other).wait_recv()
            pass_on(m, other, 0, mate, other).start()

    def relayed(m):
        for other in others:
            far = other + 1 - 2 * side
            pass_on(m, far, 0, mate, far).wait_recv()
            pass_on(m, far, 1, other, far).wait_recv()

    for m in range(kinds):
        relay(m)
    for j in range(1, ncol):
        peer, where = col_at(j)
        remote(corr_col.at[c], corr_col.at[peer], cc_send.at[peer], cc_recv.at[peer], where).wait_recv()
    corr_row[r] = jnp.sum(corr_col[...], axis=0)
    for j in range(1, nrow):
        peer, where = row_at(j)
        remote(corr_row.at[r], corr_row.at[r], cr_send.at[peer], cr_recv.at[r], where).start()
    for m in range(kinds):
        relayed(m)

    def products(k, dst):
        for m in range(kinds):
            chunk_copy(m, k).wait()
        for t in range(cap):
            g = k * cap + t
            at = picks_ref[g]
            x = jnp.concatenate([cols[m, at] for m in range(kinds)], axis=1)
            w = jnp.concatenate([tiles[m, g] for m in range(kinds)], axis=1)
            dst[k, t] = lax.dot_general(x, w, NT, preferred_element_type=F32).astype(BF16)

    def box_copy(k, where):
        return remote(outbox.at[k], inbox.at[c], box_send.at[k], box_recv.at[c], where)

    def chunk(j, carry):
        k, where = col_at(j)
        products(k, outbox)
        box_copy(k, where).start()
        return carry

    lax.fori_loop(1, ncol, chunk, 0)
    products(c, inbox)

    for j in range(1, ncol):
        peer, where = col_at(j)
        remote(seg_out.at[peer], seg_in.at[peer], seg_send.at[peer], seg_recv.at[peer], where).wait_recv()
    line = seg_in[0]
    for k in range(1, ncol):
        line = jnp.where(lax.div(slot, cap) == k, seg_in[k], line)
    here = lax.broadcasted_iota(jnp.int32, (region, tpd), 0) + c * region
    onehot = (line[:, :tpd] == here).astype(F32).astype(BF16)

    for j in range(1, nrow):
        peer, where = row_at(j)
        remote(corr_row.at[r], corr_row.at[peer], cr_send.at[peer], cr_recv.at[peer], where).wait_recv()
    corr = jnp.sum(corr_row[...], axis=0) / entries
    corr = jnp.concatenate([corr[:, i * krylov : (i + 1) * krylov] for i in range(folds)], axis=0)[:krylov]
    eye = (
        lax.broadcasted_iota(jnp.int32, (krylov, krylov), 0) == lax.broadcasted_iota(jnp.int32, (krylov, krylov), 1)
    ).astype(F32)
    once = eye - corr
    both = eye + once
    kern = exact(both, eye + exact(once, once))

    for j in range(1, ncol):
        peer, where = col_at(j)
        remote(outbox.at[peer], inbox.at[peer], box_send.at[peer], box_recv.at[peer], where).wait_recv()
    spread[...] = inbox[...].astype(F32).reshape(tpd, bs, tile)
    for b in range(bs):
        app[:, b, :] = jnp.dot(onehot, spread[:, b, :].astype(BF16), preferred_element_type=F32)
    applied = jnp.concatenate([app[s] for s in range(region)], axis=1)

    split = pieces(applied)
    raw = fold(lax.dot_general(split, basis[...], NT, preferred_element_type=F32), bs)
    energy = fold(lax.dot_general(split, split, NT, preferred_element_type=F32), bs)
    energy = energy[:, :bs] + energy[:, bs : 2 * bs] + energy[:, 2 * bs :]
    tail_col[c] = jnp.concatenate([raw, energy, jnp.zeros((bs, 128 - krylov - bs), F32)], axis=1)
    for j in range(1, ncol):
        peer, where = col_at(j)
        remote(tail_col.at[c], tail_col.at[c], tc_send.at[peer], tc_recv.at[c], where).start()
    for j in range(1, ncol):
        peer, where = col_at(j)
        remote(tail_col.at[c], tail_col.at[peer], tc_send.at[peer], tc_recv.at[peer], where).wait_recv()
    tail_row[r] = jnp.sum(tail_col[...], axis=0)
    for j in range(1, nrow):
        peer, where = row_at(j)
        remote(tail_row.at[r], tail_row.at[r], tr_send.at[peer], tr_recv.at[r], where).start()
    for j in range(1, nrow):
        peer, where = row_at(j)
        remote(tail_row.at[r], tail_row.at[peer], tr_send.at[peer], tr_recv.at[peer], where).wait_recv()
    total = jnp.sum(tail_row[...], axis=0)

    first = total[:, :krylov] * inverse_root
    coefficients = exact(first, both)
    gram = (total[:, krylov : krylov + bs] - exact(exact(first, kern), first, NT)) / entries
    coef_ref[...] = coefficients

    sub = lax.broadcasted_iota(jnp.int32, (bs, bs), 0)
    lane = lax.broadcasted_iota(jnp.int32, (bs, bs), 1)
    up = lax.broadcasted_iota(jnp.int32, (bs, 1), 0)
    factor = jnp.zeros((bs, bs), F32)
    inverse = jnp.zeros((bs, 1), F32)
    steps = []
    for j in range(bs):
        column, line = gram[:, j : j + 1], gram[j : j + 1, :]
        pivot = jnp.sqrt(gram[j : j + 1, j : j + 1])
        column = jnp.where(up >= j, column / pivot, 0.0)
        factor = jnp.where(lane == j, column, factor)
        inverse = jnp.where(up == j, 1.0 / pivot, inverse)
        steps.append(jnp.where(up > j, column, 0.0))
        gram = gram - column * (line / pivot)
    factor_ref[...] = factor

    cleaned = applied - fold(
        jnp.dot(pieces(coefficients * inverse_root), basis[...], preferred_element_type=F32), bs
    )
    solved = cleaned * inverse
    for j in range(bs - 1):
        solved = solved - (steps[j] * inverse) * solved[j : j + 1, :]
    new_ref[...] = solved

    for m in range(kinds):
        for peer in direct:
            series_copy(m, r, peer).wait_send()
        for other in others:
            pass_on(m, mate, 1, other, other).wait_send()
            pass_on(m, other, 0, mate, other).wait_send()
    for j in range(1, ncol):
        peer, where = col_at(j)
        remote(seg_out.at[peer], seg_in.at[c], seg_send.at[peer], seg_recv.at[c], where).wait_send()
        remote(corr_col.at[c], corr_col.at[c], cc_send.at[peer], cc_recv.at[c], where).wait_send()
        box_copy(peer, where).wait_send()
        remote(tail_col.at[c], tail_col.at[c], tc_send.at[peer], tc_recv.at[c], where).wait_send()
    for j in range(1, nrow):
        peer, where = row_at(j)
        remote(corr_row.at[r], corr_row.at[r], cr_send.at[peer], cr_recv.at[r], where).wait_send()
        remote(tail_row.at[r], tail_row.at[r], tr_send.at[peer], tr_recv.at[r], where).wait_send()


def shards(basis, expand, tiles, tile_rows, tile_cols):
    nrow = lax.axis_size("row")
    ncol = lax.axis_size("col")
    krylov, length = basis.shape
    kinds, tpd, tile, _ = tiles.shape
    bs = expand.shape[1]
    region = length // tile
    cap = tpd // ncol
    width = -(-tpd // 128) * 128
    dma = pltpu.SemaphoreType.DMA
    band = 16
    lanes = -(-(-(-krylov // band) * krylov) // 128) * 128
    vmem, hbm = pl.BlockSpec(memory_space=pltpu.VMEM), pl.BlockSpec(memory_space=pltpu.HBM)
    return pl.pallas_call(
        functools.partial(kernel, nrow, ncol),
        out_shape=(
            jax.ShapeDtypeStruct((bs, length), F32),
            jax.ShapeDtypeStruct((bs, krylov), F32),
            jax.ShapeDtypeStruct((bs, bs), F32),
        ),
        in_specs=[hbm] * 5,
        out_specs=(vmem, vmem, vmem),
        scratch_shapes=[
            pltpu.VMEM(expand.shape, F32),
            pltpu.SMEM((tpd,), jnp.int32),
            pltpu.SMEM((tpd,), jnp.int32),
            pltpu.VMEM((krylov, length), BF16),
            pltpu.VMEM((kinds, tpd, tile, tile), BF16),
            pltpu.VMEM((kinds, nrow * region, bs, tile), BF16),
            pltpu.VMEM((ncol, cap, bs, tile), BF16),
            pltpu.VMEM((ncol, cap, bs, tile), BF16),
            pltpu.VMEM((ncol, 1, width), jnp.int32),
            pltpu.VMEM((ncol, 1, width), jnp.int32),
            pltpu.VMEM((ncol, band, lanes), F32),
            pltpu.VMEM((nrow, band, lanes), F32),
            pltpu.VMEM((ncol, bs, 128), F32),
            pltpu.VMEM((nrow, bs, 128), F32),
            pltpu.VMEM((tpd, bs, tile), F32),
            pltpu.VMEM((region, bs, tile), F32),
            dma((3,)),
            dma,
            dma((kinds, ncol)),
            dma((kinds, nrow)),
            dma((kinds, nrow)),
            dma((kinds, nrow, 2)),
            dma((kinds, nrow, 2)),
            dma((ncol,)),
            dma((ncol,)),
            dma((ncol,)),
            dma((ncol,)),
            dma((ncol,)),
            dma((ncol,)),
            dma((nrow,)),
            dma((nrow,)),
            dma((ncol,)),
            dma((ncol,)),
            dma((nrow,)),
            dma((nrow,)),
        ],
        compiler_params=pltpu.CompilerParams(
            collective_id=0, has_side_effects=True, vmem_limit_bytes=48 * 1024 * 1024
        ),
    )(*(pltpu.with_memory_space_constraint(x, pltpu.HBM) for x in (expand, tile_rows, tile_cols, basis, tiles)))


def solution(mesh):
    return jax.shard_map(
        shards,
        mesh=mesh,
        in_specs=(
            P(None, ("row", "col")),
            P(),
            P(None, ("row", "col"), None, None),
            P(("row", "col")),
            P(("row", "col")),
        ),
        out_specs=(P(None, ("row", "col")), P(), P()),
        check_vma=False,
    )
```
